32 devices in a mesh: gx: 4 (over z), gy: 4 (over y, core), gz: 2 (over x).
Axes of the slice: x: 2, y: 2, z: 4, core: 2. Of those that a mesh axis runs over, the one named last changes fastest.
Arguments:
- right_side: float32 [128, 128, 256], P('gx', 'gy', 'gz'), may hold values from -8 to 8
- guess: float32 [128, 128, 256], P('gx', 'gy', 'gz'), may hold values from -4 to 4
Outputs:
- solution_field: float32 [128, 128, 256], P('gx', 'gy', 'gz')
- residual: float32 [128, 128, 256], P('gx', 'gy', 'gz')
The draws below stay inside these ranges and needn't reach their ends.
All inputs are finite; a program needn't handle non-finite values.
Results may differ from the reference program's by a relative error of at most 0.0001.
Values sent between devices are 32-bit elements; how exact they have to be, the bound alone decides.
No kernel may reach another device: no remote copies, remote signals or barrier semaphores. Data moves between devices by JAX's collectives and lax.ppermute only.
A program may use at most 128 MiB of HBM per device.

```python
import jax
import jax.numpy as jnp

LEVELS = 6
SWEEPS = 4
STEPS = 2
NX = 128
NY = 128
NZ = 256


def level_of(stream_key, dims, cuts, low, largest):
    level = 1.0
    for position, shards_of in cuts:
        heights = jax.random.uniform(jax.random.fold_in(jax.random.fold_in(stream_key, 6), position), (shards_of,), jnp.float32, low / len(cuts), largest / len(cuts))
        level = level * jnp.repeat(jnp.exp(heights), dims[position] // shards_of).reshape((-1,) + (1,) * (len(dims) - 1 - position))
    return level


def centred(own_key, shape, width, limit, pieces=(), kind=jnp.bfloat16):
    drawn = width * jax.random.normal(own_key, shape, jnp.float32)
    if pieces:
        drawn = drawn * level_of(own_key, shape, pieces, -0.22, 0.18)
    return jnp.clip(drawn, -limit, limit).astype(kind)


def setup_inputs(seed: int = 0) -> dict:
    keys = jax.random.split(jax.random.key(seed), 3)
    return {
        "right_side": centred(keys[0], (NX, NY, NZ), 1.0, 8.0, ((0, 4), (1, 4), (2, 2)), jnp.float32),
        "guess": centred(keys[1], (NX, NY, NZ), 0.5, 4.0, ((0, 4), (1, 4), (2, 2)), jnp.float32),
    }


damping = 2.0 / 3.0


def stencil(field):
    padded = jnp.pad(field, 1)
    beside = padded[2:, 1:-1, 1:-1] + padded[:-2, 1:-1, 1:-1]
    beside = beside + padded[1:-1, 2:, 1:-1] + padded[1:-1, :-2, 1:-1]
    beside = beside + padded[1:-1, 1:-1, 2:] + padded[1:-1, 1:-1, :-2]
    return 6.0 * field - beside


def restrict(field):
    first, second, third = field.shape
    blocks = field.reshape(first // 2, 2, second // 2, 2, third // 2, 2)
    return jnp.mean(blocks, axis=(1, 3, 5))


def prolong(field):
    first, second, third = field.shape
    spread = jnp.broadcast_to(field[:, None, :, None, :, None], (first, 2, second, 2, third, 2))
    return spread.reshape(first * 2, second * 2, third * 2)


def smooth(rhs, level_index):
    scaling = 0.25 ** level_index
    diagonal_value = 6.0 * scaling
    approx = damping * rhs / diagonal_value
    for sweep_index in range(SWEEPS - 1):
        approx = approx + damping * (rhs - scaling * stencil(approx)) / diagonal_value
    return approx


def precondition(residual):
    chain = [residual]
    for level_index in range(1, LEVELS):
        chain.append(restrict(chain[-1]))
    correction = smooth(chain[LEVELS - 1], LEVELS - 1)
    for level_index in range(LEVELS - 2, -1, -1):
        correction = prolong(correction) + smooth(chain[level_index], level_index)
    return correction


def reference(right_side, guess):
    solution_field = guess
    residual = right_side - stencil(guess)
    for step_index in range(STEPS):
        direction = precondition(residual)
        image = stencil(direction)
        alpha = jnp.sum(residual * direction) / jnp.sum(direction * image)
        solution_field = solution_field + alpha * direction
        residual = residual - alpha * image
    return solution_field, residual
```

```python
import jax
import jax.numpy as jnp
from jax import lax
from jax.experimental import pallas as pl
from jax.experimental.pallas import tpu as pltpu
from jax.sharding import PartitionSpec as P

LEVELS = 6
SWEEPS = 4
STEPS = 2
M = SWEEPS
HALO_LEVELS = 3
AXES = ("gx", "gy", "gz")
F32 = jnp.float32
HI = lax.Precision.HIGHEST


def up_to(value, unit):
    return -(-value // unit) * unit


def dot(a, b, dims=((1,), (0,))):
    return lax.dot_general(a, b, (dims, ((), ())), precision=HI, preferred_element_type=F32)


def iota(shape, dim):
    return lax.broadcasted_iota(jnp.int32, shape, dim)


def one(cond):
    return jnp.where(cond, 1.0, 0.0).astype(F32)


def signed(index, size, own):
    return jnp.where(index < own + M, index, index - size)


def cyclic(value, axis, by):
    count = lax.axis_size(axis)
    return lax.ppermute(value, axis, [(i, (i + by) % count) for i in range(count)])


class Plan:
    def __init__(self, local, counts):
        self.local, self.counts = local, counts
        self.own = [tuple(n >> l for n in local) for l in range(LEVELS)]
        self.whole = [tuple(n * c >> l for n, c in zip(local, counts)) for l in range(LEVELS)]
        self.lanes = up_to(local[2], 128)
        self.ring = []
        for l in range(LEVELS):
            if l < HALO_LEVELS:
                n = self.own[l]
                self.ring.append((n[0] + 2 * M, up_to(n[1] + 2 * M, 8), up_to(n[2] + 2 * M, 128)))
            else:
                n = self.whole[l]
                self.ring.append((n[0] + 1, up_to(n[1] + 1, 8), up_to(n[2] + 1, 128)))
        self.devices = counts[0] * counts[1] * counts[2]
        self.chunk = self.own[HALO_LEVELS][1]
        self.ext = [(n[0] + 2 * M, n[1] + 2 * M) for n in self.own[:HALO_LEVELS]]
        self.yrows = sum(n[0] * M for n in self.own[:HALO_LEVELS])
        self.xrows = sum(M * e[1] for e in self.ext)
        self.hcols = [up_to(e[0] * e[1], 128) for e in self.ext]


def restrict_to(plan, level, source, store):
    nx, ny, nz = plan.own[level]
    lanes = plan.lanes
    rz = one((iota((lanes, lanes), 0) >> 1 == iota((lanes, lanes), 1)) & (iota((lanes, lanes), 0) < nz))
    ry = one(iota((ny // 2, ny), 1) >> 1 == iota((ny // 2, ny), 0)) * 0.125
    pairs = jnp.sum(source[...].reshape(nx // 2, 2, ny, lanes), axis=1)
    across = dot(pairs.reshape(nx // 2 * ny, lanes), rz).reshape(nx // 2, ny, lanes)
    for i in range(nx // 2):
        store(i, dot(ry, across[i]))


def send_pack(plan, v, g1, g2, yl, yu, chunk, sums):
    lanes = plan.lanes

    def store1(i, u):
        g1[i] = u

    def store2(i, u):
        g2[i] = u

    restrict_to(plan, 0, v, store1)
    restrict_to(plan, 1, g1, store2)
    n3 = plan.own[3]
    parts = [jnp.zeros((n3[1], lanes), F32)]

    def store3(i, u):
        place = one(iota((lanes, lanes), 1) == iota((lanes, lanes), 0) + i * n3[2])
        place = jnp.where(iota((lanes, lanes), 0) < n3[2], place, 0.0)
        parts[0] = parts[0] + dot(u, place)

    restrict_to(plan, 2, g2, store3)
    payload = parts[0]
    if sums is not None:
        at = iota(payload.shape, 1)
        first = iota(payload.shape, 0) == 0
        payload = jnp.where((at == lanes - 2) & first, sums[0], payload)
        payload = jnp.where((at == lanes - 1) & first, sums[1], payload)
    for d in range(plan.devices):
        chunk[d * plan.chunk : (d + 1) * plan.chunk, :] = payload
    row = 0
    for l, f in enumerate((v, g1, g2)):
        nx, ny, _ = plan.own[l]
        for i in range(nx):
            yl[row : row + M, :] = f[i, 0:M, :]
            yu[row : row + M, :] = f[i, ny - M : ny, :]
            row += M


def inside(plan, idx, level, dim, ring_index):
    size = plan.ring[level][dim]
    if level < HALO_LEVELS:
        own = plan.own[level][dim]
        at = signed(ring_index, size, own) + idx[dim] * own
        ok = (at >= 0) & (at < plan.whole[level][dim])
        s = signed(ring_index, size, own)
        return ok & (s >= -M)
    return ring_index < plan.whole[level][dim]


def plane_mask(plan, idx, level):
    _, ry, rz = plan.ring[level]
    return one(
        inside(plan, idx, level, 1, iota((ry, rz), 0)) & inside(plan, idx, level, 2, iota((ry, rz), 1))
    )


def smooth(plan, idx, level, g, a, b):
    rx, ry, rz = plan.ring[level]
    m9 = plane_mask(plan, idx, level) * (1.0 / 9.0)
    source, target = g, a
    for sweep in range(SWEEPS - 1):

        def body(i, carry, source=source, target=target):
            f = source[i]
            before = source[jnp.where(i == 0, rx - 1, i - 1)]
            after = source[jnp.where(i == rx - 1, 0, i + 1)]
            beside = before + after + pltpu.roll(f, 1, 0) + pltpu.roll(f, ry - 1, 0)
            beside = beside + pltpu.roll(f, 1, 1) + pltpu.roll(f, rz - 1, 1)
            sx = one(inside(plan, idx, level, 0, i))
            target[i] = g[i] + (m9 * sx) * (3.0 * f + beside)
            return carry

        lax.fori_loop(0, rx, body, 0)
        source, target = target, (b if target is a else a)
    return source


def coarse_map(plan, idx, level, dim, fine, coarse):
    size = plan.ring[level][dim]
    if level < HALO_LEVELS:
        s = signed(fine, size, plan.own[level][dim])
        if level + 1 < HALO_LEVELS:
            up = s >> 1
            return jnp.where(up < 0, up + plan.ring[level + 1][dim], up) == coarse
        return (s + idx[dim] * plan.own[level][dim]) >> 1 == coarse
    return (fine >> 1 == coarse) & (fine < plan.whole[level][dim])


def add_prolonged(plan, idx, level, f, scale, zc, out):
    rx, ry, rz = plan.ring[level]
    cx, cy, cz = plan.ring[level + 1]
    pz = one(coarse_map(plan, idx, level, 2, iota((cz, rz), 1), iota((cz, rz), 0)))
    py = one(coarse_map(plan, idx, level, 1, iota((ry, cy), 0), iota((ry, cy), 1)))
    halo = level < HALO_LEVELS
    low = -1 if halo else 0
    high = plan.own[level][0] + 1 if halo else plan.whole[level][0]
    if level + 1 == HALO_LEVELS:
        for s in range(low, high):
            i = s % rx
            at = s + idx[0] * plan.own[level][0]
            ok = (at >= 0) & (at < plan.whole[level][0])
            c = jnp.clip(at >> 1, 0, plan.whole[level + 1][0] - 1)
            u = dot(py, dot(zc[c], pz))
            out[i] = scale * f[i] + one(ok) * u
        return
    spread = dot(zc[...].reshape(cx * cy, cz), pz).reshape(cx, cy, rz)
    for c in range(low >> 1, (high - 1 >> 1) + 1):
        u = dot(py, spread[c % cx])
        for s in (2 * c, 2 * c + 1):
            if low <= s < high:
                i = s % rx
                out[i] = scale * f[i] + u
    if not halo:
        for i in range(high, rx):
            out[i] = jnp.zeros((ry, rz), F32)


def faces_kernel(plan, guess, xl, xu, yl, yu, zf):
    nx, ny, nz = plan.local
    lanes = plan.lanes
    xl[...] = guess[0]
    xu[...] = guess[nx - 1]
    yl[...] = guess[:, 0, :]
    yu[...] = guess[:, ny - 1, :]
    at, row = iota((8, lanes), 1), iota((8, lanes), 0)
    pick = one(((row == 0) & (at == 0)) | ((row == 1) & (at == nz - 1)))
    zf[...] = dot(pick, guess[...].reshape(nx * ny, lanes), ((1,), (1,)))


def residual_kernel(plan, idx, b, guess, xlo, xhi, ylo, yhi, zlo, zhi, r, g1, g2, yl, yu, chunk, side):
    nx, ny, nz = plan.local
    lanes = plan.lanes
    cx, cy, cz = plan.counts
    has = lambda dim, upper: one(idx[dim] < plan.counts[dim] - 1 if upper else idx[dim] > 0)
    at, row = iota((8, lanes), 1), iota((8, lanes), 0)
    upper = one((row == 0) & (at == nz - 1)) * has(2, True)
    lower = one((row == 1) & (at == 0)) * has(2, False)
    side[...] = (dot(zhi[...], upper, ((0,), (0,))) + dot(zlo[...], lower, ((0,), (0,)))).reshape(nx, ny, lanes)
    ys, zs = iota((ny, lanes), 0), iota((ny, lanes), 1)
    not_low, not_high = one(zs > 0), one(zs < nz - 1)
    y_low, y_high = ys == 0, ys == ny - 1
    for i in range(nx):
        f = guess[i]
        before = guess[i - 1] if i else xlo[...] * has(0, False)
        after = guess[i + 1] if i < nx - 1 else xhi[...] * has(0, True)
        beside = before + after
        beside = beside + jnp.where(y_low, (ylo[i] * has(1, False))[None, :], pltpu.roll(f, 1, 0))
        beside = beside + jnp.where(y_high, (yhi[i] * has(1, True))[None, :], pltpu.roll(f, ny - 1, 0))
        beside = beside + pltpu.roll(f, 1, 1) * not_low + pltpu.roll(f, lanes - 1, 1) * not_high
        r[i] = b[i] - (6.0 * f - (beside + side[i]))
    send_pack(plan, r, g1, g2, yl, yu, chunk, None)


def ring_y_kernel(plan, v, g1, g2, ylo, yhi, a0, a1, a2, xl, xu):
    row, out = 0, 0
    for l, (f, a) in enumerate(((v, a0), (g1, a1), (g2, a2))):
        nx, ny, _ = plan.own[l]
        e = plan.ext[l][1]
        a[:, 0:ny, :] = f[...]
        for i in range(nx):
            a[i, ny : ny + M, :] = yhi[row : row + M, :]
            a[i, ny + M : ny + 2 * M, :] = ylo[row : row + M, :]
            row += M
        for i in range(M):
            xl[out : out + e, :] = a[i]
            xu[out : out + e, :] = a[nx - M + i]
            out += e


def ring_x_kernel(plan, a0, a1, a2, xlo, xhi, c0, c1, c2, h):
    row, col = 0, 0
    lanes = plan.lanes
    at, k = iota((8, lanes), 1), iota((8, lanes), 0)
    for l, (a, c) in enumerate(((a0, c0), (a1, c1), (a2, c2))):
        nx, ny, nz = plan.own[l]
        ex, e = plan.ext[l]
        c[0:nx] = a[...]
        for i in range(M):
            c[nx + i] = xhi[row : row + e, :]
            c[nx + M + i] = xlo[row : row + e, :]
            row += e
        pick = one(at == jnp.where(k < M, k, nz - 2 * M + k))
        h[:, col : col + ex * e] = dot(pick, c[...].reshape(ex * e, lanes), ((1,), (1,)))
        if plan.hcols[l] > ex * e:
            h[:, col + ex * e : col + plan.hcols[l]] = jnp.zeros((8, plan.hcols[l] - ex * e), F32)
        col += plan.hcols[l]


def total_sums(plan, chunks):
    rows = chunks.shape
    at = iota(rows, 1)
    first = iota(rows, 0) % plan.chunk == 0
    data = chunks[...]
    along = jnp.sum(jnp.where((at == plan.lanes - 2) & first, data, 0.0))
    curvature = jnp.sum(jnp.where((at == plan.lanes - 1) & first, data, 0.0))
    return along, curvature


def step_kernel(plan, last, *refs):
    nin = 7 if not last else 11
    idx, c0, c1, c2, hlo, hhi, chunks = refs[:7]
    old = refs[7:nin]
    outs = refs[nin:]
    if last:
        z_out, w_out, sums_out = outs[:3]
        scratch = outs[3:]
        rings = scratch[:4]
        scratch = scratch[4:]
    else:
        z_out, w_out, g1, g2, yl, yu, chunk = outs[:7]
        rings = outs[7:11]
        scratch = outs[11:]
    bufs = [scratch[2 * l : 2 * l + 2] for l in range(LEVELS)]
    g4, g5 = scratch[2 * LEVELS : 2 * LEVELS + 2]
    fields = list(rings) + [g4, g5]
    lanes = plan.lanes
    if last:
        along, curvature = total_sums(plan, chunks)
        alpha = along / curvature
    col = 0
    at, k = iota((8, lanes), 1), iota((8, lanes), 0)
    for l, c in enumerate((c0, c1, c2)):
        nx, ny, nz = plan.own[l]
        ex, e = plan.ext[l]
        rx, ry, rz = plan.ring[l]
        mask = plane_mask(plan, idx, l)
        base = rz - lanes
        want = jnp.where(k < M, nz + k - base, lanes - 2 * M + k)
        place = one(at == want)
        got = jnp.where(iota((8, ex * e), 0) < M, hhi[:, col : col + ex * e], hlo[:, col : col + ex * e])
        col += plan.hcols[l]
        tile = dot(got, place, ((0,), (0,))).reshape(ex, e, lanes)
        for i in range(rx):
            m = mask * one(inside(plan, idx, l, 0, jnp.int32(i)))
            if base:
                full = jnp.concatenate([c[i], tile[i]], axis=1)
            else:
                full = c[i] + tile[i]
            full = full * m
            rings[l][i] = old[l][i] - alpha * full if last else full
    n3 = plan.own[3]
    g3 = rings[3]
    g3[...] = jnp.zeros(g3.shape, F32)
    d = 0
    for ix in range(plan.counts[0]):
        for iy in range(plan.counts[1]):
            for iz in range(plan.counts[2]):
                part = chunks[d * plan.chunk : (d + 1) * plan.chunk, :]
                for i in range(n3[0]):
                    g3[
                        ix * n3[0] + i, iy * n3[1] : (iy + 1) * n3[1], iz * n3[2] : (iz + 1) * n3[2]
                    ] = part[:, i * n3[2] : (i + 1) * n3[2]]
                d += 1
    if last:
        g3[...] = old[3][...] - alpha * g3[...]
    for l in (3, 4):
        rx, ry, rz = plan.ring[l]
        cx, cy, cz = plan.ring[l + 1]
        rzm = one((iota((rz, cz), 0) >> 1 == iota((rz, cz), 1)) & (iota((rz, cz), 0) < plan.whole[l][2]))
        rym = one((iota((cy, ry), 1) >> 1 == iota((cy, ry), 0)) & (iota((cy, ry), 1) < plan.whole[l][1])) * 0.125
        for i in range(plan.whole[l + 1][0]):
            fields[l + 1][i] = dot(rym, dot(fields[l][2 * i] + fields[l][2 * i + 1], rzm))
        fields[l + 1][cx - 1] = jnp.zeros((cy, cz), F32)
    zc = None
    for l in range(LEVELS - 1, -1, -1):
        f = smooth(plan, idx, l, fields[l], *bufs[l])
        out = bufs[l][1] if f is bufs[l][0] else bufs[l][0]
        scale = 4.0**l / 9.0
        if zc is None:
            out[...] = scale * f[...]
        else:
            add_prolonged(plan, idx, l, f, scale, zc, out)
        zc = out
    nx, ny, nz = plan.local
    rx, ry, rz = plan.ring[0]
    first = jnp.zeros((ny, lanes), F32)
    second = jnp.zeros((ny, lanes), F32)

    def body(i, carry):
        first, second = carry
        f = zc[i]
        before = zc[jnp.where(i == 0, rx - 1, i - 1)]
        after = zc[i + 1]
        beside = before + after + pltpu.roll(f, 1, 0) + pltpu.roll(f, ry - 1, 0)
        beside = beside + pltpu.roll(f, 1, 1) + pltpu.roll(f, rz - 1, 1)
        w = (6.0 * f - beside)[:ny, :lanes]
        z = f[:ny, :lanes]
        z_out[i] = z
        w_out[i] = w
        return first + z * rings[0][i][:ny, :lanes], second + z * w

    first, second = lax.fori_loop(0, nx, body, (first, second))
    sums = (jnp.sum(first), jnp.sum(second))
    if last:
        row, at = iota(sums_out.shape, 0), iota(sums_out.shape, 1)
        sums_out[...] = jnp.where(at == lanes - 2, sums[0], jnp.where(at == lanes - 1, sums[1], 0.0))
    else:
        send_pack(plan, w_out, g1, g2, yl, yu, chunk, sums)


def final_kernel(plan, chunks1, chunks2, guess, r, z1, w1, z2, w2, x_out, r_out):
    along, curvature = total_sums(plan, chunks1)
    alpha1 = along / curvature
    data = chunks2[...]
    at = iota(data.shape, 1)
    along = jnp.sum(jnp.where(at == plan.lanes - 2, data, 0.0))
    curvature = jnp.sum(jnp.where(at == plan.lanes - 1, data, 0.0))
    alpha2 = along / curvature
    x_out[...] = guess[...] + alpha1 * z1[...] + alpha2 * z2[...]
    r_out[...] = r[...] - alpha1 * w1[...] - alpha2 * w2[...]


def sds(*shape):
    return jax.ShapeDtypeStruct(shape, F32)


def call(body, outs, args, scratch=(), smem=False):
    specs = [pl.BlockSpec(memory_space=pltpu.VMEM)] * len(args)
    if smem:
        specs[0] = pl.BlockSpec(memory_space=pltpu.SMEM)
    return pl.pallas_call(
        body,
        out_shape=tuple(outs),
        in_specs=specs,
        out_specs=tuple(pl.BlockSpec(memory_space=pltpu.VMEM) for _ in outs),
        scratch_shapes=list(scratch),
    )(*args)


def exchange(value_low, value_high, axis):
    return cyclic(value_high, axis, 1), cyclic(value_low, axis, -1)


def shards(right_side, guess):
    counts = tuple(lax.axis_size(a) for a in AXES)
    plan = Plan(right_side.shape, counts)
    nx, ny, nz = plan.local
    lanes = plan.lanes
    idx = jnp.stack([lax.axis_index(a) for a in AXES]).astype(jnp.int32)
    bind = lambda f, *extra: lambda *refs: f(plan, *extra, *refs)
    own = [sds(*n[:2], lanes) for n in plan.own[:HALO_LEVELS]]
    packs = [own[1], own[2], sds(plan.yrows, lanes), sds(plan.yrows, lanes), sds(plan.devices * plan.chunk, lanes)]

    xl, xu, yl, yu, zf = call(
        bind(faces_kernel), [sds(ny, lanes), sds(ny, lanes), sds(nx, lanes), sds(nx, lanes), sds(8, nx * ny)], [guess]
    )
    xlo, xhi = exchange(xl, xu, "gx")
    ylo, yhi = exchange(yl, yu, "gy")
    zlo, zhi = swap(zf)
    r, g1, g2, yl, yu, chunk = call(
        bind(residual_kernel),
        [own[0]] + packs,
        [idx, right_side, guess, xlo, xhi, ylo, yhi, zlo, zhi],
        [pltpu.VMEM((nx, ny, lanes), F32)],
        smem=True,
    )
    rings = [sds(*s) for s in plan.ring[:4]]
    as_scratch = lambda items: [pltpu.VMEM(s.shape, F32) for s in items]
    work = [pltpu.VMEM(s, F32) for s in plan.ring for _ in range(2)]
    work += [pltpu.VMEM(s, F32) for s in plan.ring[4:6]]
    field, old = r, []
    kept = []
    for step in range(STEPS):
        last = step == STEPS - 1
        chunks = lax.all_to_all(chunk, AXES, 0, 0, tiled=True)
        ylo, yhi = exchange(yl, yu, "gy")
        *a, xl, xu = call(
            bind(ring_y_kernel),
            [sds(n[0], e[1], lanes) for n, e in zip(plan.own, plan.ext)] + [sds(plan.xrows, lanes)] * 2,
            [field, g1, g2, ylo, yhi],
        )
        xlo, xhi = exchange(xl, xu, "gx")
        *c, h = call(
            bind(ring_x_kernel),
            [sds(*e, lanes) for e in plan.ext] + [sds(8, sum(plan.hcols))],
            [*a, xlo, xhi],
        )
        hlo, hhi = swap(h)
        args = [idx, *c, hlo, hhi, chunks, *old]
        if last:
            z, w, sums = call(
                bind(step_kernel, True), [own[0], own[0], sds(plan.devices, lanes)], args, as_scratch(rings) + work, smem=True
            )
        else:
            z, w, g1, g2, yl, yu, chunk, *old = call(
                bind(step_kernel, False), [own[0], own[0]] + packs + rings, args, work, smem=True
            )
            field = w
        kept.append((z, w, chunks))
    sums = lax.all_to_all(sums, AXES, 0, 0, tiled=True)
    (z1, w1, _), (z2, w2, chunks1) = kept
    return call(bind(final_kernel), [own[0], own[0]], [chunks1, sums, guess, r, z1, w1, z2, w2])


def swap(h):
    low = cyclic(h, "gz", 1)
    return (low, low) if lax.axis_size("gz") == 2 else (low, cyclic(h, "gz", -1))


def solution(mesh):
    placed = P("gx", "gy", "gz")
    return jax.shard_map(shards, mesh=mesh, in_specs=(placed, placed), out_specs=(placed, placed), check_vma=False)
```

```python
import jax
import jax.numpy as jnp
from jax import lax
from jax.experimental import pallas as pl
from jax.experimental.pallas import tpu as pltpu
from jax.sharding import PartitionSpec as P

LEVELS = 6
SWEEPS = 4
STEPS = 2
M = SWEEPS
HALO_LEVELS = 3
AXES = ("gx", "gy", "gz")
F32 = jnp.float32
UNROLL = 24 * 24 * 128
HI = lax.Precision.HIGHEST


def up_to(value, unit):
    return -(-value // unit) * unit


def dot(a, b, dims=((1,), (0,))):
    return lax.dot_general(a, b, (dims, ((), ())), precision=HI, preferred_element_type=F32)


def halves(x):
    high = x.astype(jnp.bfloat16).astype(F32)
    return high, x - high


def dot_right(x, hot):
    both = jnp.concatenate(halves(x), axis=1).astype(jnp.bfloat16)
    return lax.dot_general(
        both, jnp.concatenate([hot, hot], axis=0).astype(jnp.bfloat16), (((1,), (0,)), ((), ())), preferred_element_type=F32
    )


def dot_pick(hot, x):
    both = jnp.concatenate(halves(x), axis=1).astype(jnp.bfloat16)
    return lax.dot_general(
        jnp.concatenate([hot, hot], axis=1).astype(jnp.bfloat16), both, (((1,), (1,)), ((), ())), preferred_element_type=F32
    )


def dot_place(x, hot):
    both = jnp.concatenate(halves(x), axis=0).astype(jnp.bfloat16)
    return lax.dot_general(
        both, jnp.concatenate([hot, hot], axis=0).astype(jnp.bfloat16), (((0,), (0,)), ((), ())), preferred_element_type=F32
    )


def iota(shape, dim):
    return lax.broadcasted_iota(jnp.int32, shape, dim)


def one(cond):
    return jnp.where(cond, 1.0, 0.0).astype(F32)


def signed(index, size, own):
    return jnp.where(index < own + M, index, index - size)


def cyclic(value, axis, by):
    count = lax.axis_size(axis)
    return lax.ppermute(value, axis, [(i, (i + by) % count) for i in range(count)])


class Plan:
    def __init__(self, local, counts):
        self.local, self.counts = local, counts
        self.own = [tuple(n >> l for n in local) for l in range(LEVELS)]
        self.whole = [tuple(n * c >> l for n, c in zip(local, counts)) for l in range(LEVELS)]
        self.lanes = up_to(local[2], 128)
        self.ring = []
        for l in range(LEVELS):
            if l < HALO_LEVELS:
                n = self.own[l]
                self.ring.append((n[0] + 2 * M, up_to(n[1] + 2 * M, 8), up_to(n[2] + 2 * M, 128)))
            else:
                n = self.whole[l]
                self.ring.append((n[0] + 1, up_to(n[1] + 1, 8), up_to(n[2] + 1, 128)))
        self.devices = counts[0] * counts[1] * counts[2]
        self.chunk = self.own[HALO_LEVELS][1]
        self.ext = [(n[0] + 2 * M, n[1] + 2 * M) for n in self.own[:HALO_LEVELS]]
        self.tmp = pltpu.VMEM(
            (max(r[0] for r in self.ring), max(r[1] for r in self.ring), 128), F32
        )
        self.yrows = sum(n[0] * M for n in self.own[:HALO_LEVELS])
        self.xrows = sum(M * e[1] for e in self.ext)
        self.hcols = [up_to(e[0] * e[1], 128) for e in self.ext]


def restrict_to(plan, level, source, tmp):
    nx, ny, nz = plan.own[level]
    lanes = plan.lanes
    rz = one((iota((lanes, lanes), 0) >> 1 == iota((lanes, lanes), 1)) & (iota((lanes, lanes), 0) < nz)) * 0.125
    hx, hy = nx // 2, ny // 2
    for i in range(hx):
        tmp[i, 0:ny, 0:lanes] = source[2 * i] + source[2 * i + 1]
    pairs = tmp[0:hx, pl.ds(0, hy, stride=2), 0:lanes] + tmp[0:hx, pl.ds(1, hy, stride=2), 0:lanes]
    if hy % 8:
        return jnp.stack([dot_right(pairs[i], rz) for i in range(hx)])
    return dot_right(pairs.reshape(hx * hy, lanes), rz).reshape(hx, hy, lanes)


def send_pack(plan, v, g1, g2, yl, yu, chunk, sums, tmp):
    lanes = plan.lanes
    g1[...] = restrict_to(plan, 0, v, tmp)
    g2[...] = restrict_to(plan, 1, g1, tmp)
    n3 = plan.own[3]
    coarse = restrict_to(plan, 2, g2, tmp)
    parts = [jnp.zeros((n3[1], lanes), F32)]
    for i in range(n3[0]):
        parts[0] = parts[0] + (pltpu.roll(coarse[i], i * n3[2], 1) if i else coarse[i])
    payload = parts[0]
    if sums is not None:
        at = iota(payload.shape, 1)
        first = iota(payload.shape, 0) == 0
        payload = jnp.where((at == lanes - 2) & first, sums[0], payload)
        payload = jnp.where((at == lanes - 1) & first, sums[1], payload)
    for d in range(plan.devices):
        chunk[d * plan.chunk : (d + 1) * plan.chunk, :] = payload
    row = 0
    for l, f in enumerate((v, g1, g2)):
        nx, ny, _ = plan.own[l]
        for i in range(nx):
            yl[row : row + M, :] = f[i, 0:M, :]
            yu[row : row + M, :] = f[i, ny - M : ny, :]
            row += M


def inside(plan, idx, level, dim, ring_index):
    size = plan.ring[level][dim]
    if level < HALO_LEVELS:
        own = plan.own[level][dim]
        at = signed(ring_index, size, own) + idx[dim] * own
        ok = (at >= 0) & (at < plan.whole[level][dim])
        s = signed(ring_index, size, own)
        return ok & (s >= -M)
    return ring_index < plan.whole[level][dim]


def plane_mask(plan, idx, level):
    _, ry, rz = plan.ring[level]
    return one(
        inside(plan, idx, level, 1, iota((ry, rz), 0)) & inside(plan, idx, level, 2, iota((ry, rz), 1))
    )


def smooth(plan, idx, level, g, a, b):
    rx, ry, rz = plan.ring[level]
    m9 = plane_mask(plan, idx, level) * (1.0 / 9.0)
    source, target = g, a
    for sweep in range(SWEEPS - 1):

        group = rx if rx * ry * rz <= UNROLL else max(u for u in range(1, 9) if rx % u == 0)

        def plane(i, source=source, target=target):
            fixed = isinstance(i, int)
            f = source[i]
            before = source[(i - 1) % rx if fixed else jnp.where(i == 0, rx - 1, i - 1)]
            after = source[(i + 1) % rx if fixed else jnp.where(i == rx - 1, 0, i + 1)]
            beside = before + after + pltpu.roll(f, 1, 0) + pltpu.roll(f, ry - 1, 0)
            beside = beside + pltpu.roll(f, 1, 1) + pltpu.roll(f, rz - 1, 1)
            sx = one(inside(plan, idx, level, 0, jnp.int32(i)))
            target[i] = g[i] + (m9 * sx) * (3.0 * f + beside)

        def body(j, carry, plane=plane, group=group):
            for u in range(group):
                plane(j * group + u)
            return carry

        if group == rx:
            for i in range(rx):
                plane(i)
        else:
            lax.fori_loop(0, rx // group, body, 0)
        source, target = target, (b if target is a else a)
    return source


def coarse_map(plan, idx, level, dim, fine, coarse):
    size = plan.ring[level][dim]
    if level < HALO_LEVELS:
        s = signed(fine, size, plan.own[level][dim])
        if level + 1 < HALO_LEVELS:
            up = s >> 1
            return jnp.where(up < 0, up + plan.ring[level + 1][dim], up) == coarse
        return (s + idx[dim] * plan.own[level][dim]) >> 1 == coarse
    return (fine >> 1 == coarse) & (fine < plan.whole[level][dim])


def add_prolonged(plan, idx, level, f, scale, zc, out, tmp):
    rx, ry, rz = plan.ring[level]
    cx, cy, cz = plan.ring[level + 1]
    pz = one(coarse_map(plan, idx, level, 2, iota((cz, rz), 1), iota((cz, rz), 0)))
    halo = level < HALO_LEVELS
    low = -1 if halo else 0
    high = plan.own[level][0] + 1 if halo else plan.whole[level][0]
    planes = range(low >> 1, (high - 1 >> 1) + 1)
    if level + 1 == HALO_LEVELS:
        py = one(coarse_map(plan, idx, level, 1, iota((ry, cy), 0), iota((ry, cy), 1)))
        for k in planes:
            at = k + idx[0] * (plan.own[level][0] // 2)
            ok = (at >= 0) & (at < plan.whole[level + 1][0])
            c = jnp.clip(at, 0, plan.whole[level + 1][0] - 1)
            u = dot(py, dot_right(zc[c], pz)) * one(ok)
            for s in (2 * k, 2 * k + 1):
                if low <= s < high:
                    out[s % rx] = scale * f[s % rx] + u
        return
    upper = (plan.own[level][1] + M) // 2 if halo else ry // 2
    for n, k in enumerate(planes):
        for odd in (0, 1):
            tmp[n, pl.ds(odd, upper, stride=2), 0:cz] = zc[k % cx, 0:upper, :]
            if halo:
                tmp[n, pl.ds(2 * upper + odd, M // 2, stride=2), 0:cz] = zc[k % cx, cy - M // 2 : cy, :]
    spread = dot_right(tmp[0 : len(planes), 0:ry, 0:cz].reshape(len(planes) * ry, cz), pz).reshape(len(planes), ry, rz)
    for n, k in enumerate(planes):
        for s in (2 * k, 2 * k + 1):
            if low <= s < high:
                out[s % rx] = scale * f[s % rx] + spread[n]
    if not halo:
        for i in range(high, rx):
            out[i] = jnp.zeros((ry, rz), F32)


def faces_kernel(plan, guess, xl, xu, yl, yu, zf):
    nx, ny, nz = plan.local
    lanes = plan.lanes
    xl[...] = guess[0]
    xu[...] = guess[nx - 1]
    yl[...] = guess[:, 0, :]
    yu[...] = guess[:, ny - 1, :]
    at, row = iota((8, lanes), 1), iota((8, lanes), 0)
    pick = one(((row == 0) & (at == 0)) | ((row == 1) & (at == nz - 1)))
    zf[...] = dot_pick(pick, guess[...].reshape(nx * ny, lanes))


def residual_kernel(plan, idx, b, guess, xlo, xhi, ylo, yhi, zlo, zhi, r, g1, g2, yl, yu, chunk, side, tmp):
    nx, ny, nz = plan.local
    lanes = plan.lanes
    cx, cy, cz = plan.counts
    has = lambda dim, upper: one(idx[dim] < plan.counts[dim] - 1 if upper else idx[dim] > 0)
    at, row = iota((8, lanes), 1), iota((8, lanes), 0)
    upper = one((row == 0) & (at == nz - 1)) * has(2, True)
    lower = one((row == 1) & (at == 0)) * has(2, False)
    got = jnp.where(iota((8, nx * ny), 0) == 0, zhi[...], zlo[...])
    side[...] = dot_place(got, upper + lower).reshape(nx, ny, lanes)
    ys, zs = iota((ny, lanes), 0), iota((ny, lanes), 1)
    not_low, not_high = one(zs > 0), one(zs < nz - 1)
    y_low, y_high = ys == 0, ys == ny - 1
    for i in range(nx):
        f = guess[i]
        before = guess[i - 1] if i else xlo[...] * has(0, False)
        after = guess[i + 1] if i < nx - 1 else xhi[...] * has(0, True)
        beside = before + after
        beside = beside + jnp.where(y_low, (ylo[i] * has(1, False))[None, :], pltpu.roll(f, 1, 0))
        beside = beside + jnp.where(y_high, (yhi[i] * has(1, True))[None, :], pltpu.roll(f, ny - 1, 0))
        beside = beside + pltpu.roll(f, 1, 1) * not_low + pltpu.roll(f, lanes - 1, 1) * not_high
        r[i] = b[i] - (6.0 * f - (beside + side[i]))
    send_pack(plan, r, g1, g2, yl, yu, chunk, None, tmp)


def ring_y_kernel(plan, v, g1, g2, ylo, yhi, a0, a1, a2, xl, xu):
    row, out = 0, 0
    for l, (f, a) in enumerate(((v, a0), (g1, a1), (g2, a2))):
        nx, ny, _ = plan.own[l]
        e = plan.ext[l][1]
        a[:, 0:ny, :] = f[...]
        for i in range(nx):
            a[i, ny : ny + M, :] = yhi[row : row + M, :]
            a[i, ny + M : ny + 2 * M, :] = ylo[row : row + M, :]
            row += M
        for i in range(M):
            xl[out : out + e, :] = a[i]
            xu[out : out + e, :] = a[nx - M + i]
            out += e


def ring_x_kernel(plan, a0, a1, a2, xlo, xhi, c0, c1, c2, h):
    row, col = 0, 0
    lanes = plan.lanes
    at, k = iota((8, lanes), 1), iota((8, lanes), 0)
    for l, (a, c) in enumerate(((a0, c0), (a1, c1), (a2, c2))):
        nx, ny, nz = plan.own[l]
        ex, e = plan.ext[l]
        c[0:nx] = a[...]
        for i in range(M):
            c[nx + i] = xhi[row : row + e, :]
            c[nx + M + i] = xlo[row : row + e, :]
            row += e
        pick = one(at == jnp.where(k < M, k, nz - 2 * M + k))
        h[:, col : col + ex * e] = dot_pick(pick, c[...].reshape(ex * e, lanes))
        if plan.hcols[l] > ex * e:
            h[:, col + ex * e : col + plan.hcols[l]] = jnp.zeros((8, plan.hcols[l] - ex * e), F32)
        col += plan.hcols[l]


def total_sums(plan, chunks):
    rows = chunks.shape
    at = iota(rows, 1)
    first = iota(rows, 0) % plan.chunk == 0
    data = chunks[...]
    along = jnp.sum(jnp.where((at == plan.lanes - 2) & first, data, 0.0))
    curvature = jnp.sum(jnp.where((at == plan.lanes - 1) & first, data, 0.0))
    return along, curvature


def step_kernel(plan, last, *refs):
    nin = 7 if not last else 11
    idx, c0, c1, c2, hlo, hhi, chunks = refs[:7]
    old = refs[7:nin]
    outs = refs[nin:]
    if last:
        z_out, w_out, sums_out = outs[:3]
        scratch = outs[3:]
        rings = scratch[:4]
        scratch = scratch[4:]
    else:
        z_out, w_out, g1, g2, yl, yu, chunk = outs[:7]
        rings = outs[7:11]
        scratch = outs[11:]
    bufs = [scratch[2 * l : 2 * l + 2] for l in range(LEVELS)]
    g4, g5, tmp = scratch[2 * LEVELS : 2 * LEVELS + 3]
    fields = list(rings) + [g4, g5]
    lanes = plan.lanes
    if last:
        along, curvature = total_sums(plan, chunks)
        alpha = along / curvature
    col = 0
    at, k = iota((8, lanes), 1), iota((8, lanes), 0)
    for l, c in enumerate((c0, c1, c2)):
        nx, ny, nz = plan.own[l]
        ex, e = plan.ext[l]
        rx, ry, rz = plan.ring[l]
        mask = plane_mask(plan, idx, l)
        base = rz - lanes
        want = jnp.where(k < M, nz + k - base, lanes - 2 * M + k)
        place = one(at == want)
        got = jnp.where(iota((8, ex * e), 0) < M, hhi[:, col : col + ex * e], hlo[:, col : col + ex * e])
        col += plan.hcols[l]
        tile = dot_place(got, place).reshape(ex, e, lanes)
        for i in range(rx):
            m = mask * one(inside(plan, idx, l, 0, jnp.int32(i)))
            if base:
                full = jnp.concatenate([c[i], tile[i]], axis=1)
            else:
                full = c[i] + tile[i]
            full = full * m
            rings[l][i] = old[l][i] - alpha * full if last else full
    n3 = plan.own[3]
    g3 = rings[3]
    g3[...] = jnp.zeros(g3.shape, F32)
    d = 0
    for ix in range(plan.counts[0]):
        for iy in range(plan.counts[1]):
            for iz in range(plan.counts[2]):
                part = chunks[d * plan.chunk : (d + 1) * plan.chunk, :]
                for i in range(n3[0]):
                    g3[
                        ix * n3[0] + i, iy * n3[1] : (iy + 1) * n3[1], iz * n3[2] : (iz + 1) * n3[2]
                    ] = part[:, i * n3[2] : (i + 1) * n3[2]]
                d += 1
    if last:
        g3[...] = old[3][...] - alpha * g3[...]
    for l in (3, 4):
        rx, ry, rz = plan.ring[l]
        cx, cy, cz = plan.ring[l + 1]
        rzm = one((iota((rz, cz), 0) >> 1 == iota((rz, cz), 1)) & (iota((rz, cz), 0) < plan.whole[l][2])) * 0.125
        hx, hy = plan.whole[l + 1][:2]
        fields[l + 1][...] = jnp.zeros((cx, cy, cz), F32)
        for i in range(hx):
            both = fields[l][2 * i] + fields[l][2 * i + 1]
            pieces = []
            for t in range(0, rz, 128):
                n = i * (rz // 128) + t // 128
                tmp[n, 0:ry, :] = both[:, t : t + 128]
                pieces.append(tmp[n, pl.ds(0, ry // 2, stride=2), :] + tmp[n, pl.ds(1, ry // 2, stride=2), :])
            pair = jnp.concatenate(pieces, axis=1)
            fields[l + 1][i, 0 : ry // 2, :] = dot_right(pair, rzm)
    zc = None
    for l in range(LEVELS - 1, -1, -1):
        f = smooth(plan, idx, l, fields[l], *bufs[l])
        out = bufs[l][1] if f is bufs[l][0] else bufs[l][0]
        scale = 4.0**l / 9.0
        if zc is None:
            out[...] = scale * f[...]
        else:
            add_prolonged(plan, idx, l, f, scale, zc, out, tmp)
        zc = out
    nx, ny, nz = plan.local
    rx, ry, rz = plan.ring[0]
    first = jnp.zeros((ny, lanes), F32)
    second = jnp.zeros((ny, lanes), F32)

    group = max(u for u in range(1, 5) if nx % u == 0)

    def body(j, carry):
        first, second = carry
        for u in range(group):
            i = j * group + u
            f = zc[i]
            before = zc[jnp.where(i == 0, rx - 1, i - 1)]
            after = zc[i + 1]
            beside = before + after + pltpu.roll(f, 1, 0) + pltpu.roll(f, ry - 1, 0)
            beside = beside + pltpu.roll(f, 1, 1) + pltpu.roll(f, rz - 1, 1)
            w = (6.0 * f - beside)[:ny, :lanes]
            z = f[:ny, :lanes]
            z_out[i] = z
            w_out[i] = w
            first = first + z * rings[0][i][:ny, :lanes]
            second = second + z * w
        return first, second

    first, second = lax.fori_loop(0, nx // group, body, (first, second))
    sums = (jnp.sum(first), jnp.sum(second))
    if last:
        row, at = iota(sums_out.shape, 0), iota(sums_out.shape, 1)
        sums_out[...] = jnp.where(at == lanes - 2, sums[0], jnp.where(at == lanes - 1, sums[1], 0.0))
    else:
        send_pack(plan, w_out, g1, g2, yl, yu, chunk, sums, tmp)


def final_kernel(plan, chunks1, chunks2, guess, r, z1, w1, z2, w2, x_out, r_out):
    along, curvature = total_sums(plan, chunks1)
    alpha1 = along / curvature
    data = chunks2[...]
    at = iota(data.shape, 1)
    along = jnp.sum(jnp.where(at == plan.lanes - 2, data, 0.0))
    curvature = jnp.sum(jnp.where(at == plan.lanes - 1, data, 0.0))
    alpha2 = along / curvature
    x_out[...] = guess[...] + alpha1 * z1[...] + alpha2 * z2[...]
    r_out[...] = r[...] - alpha1 * w1[...] - alpha2 * w2[...]


def sds(*shape):
    return jax.ShapeDtypeStruct(shape, F32)


def call(body, outs, args, scratch=(), smem=False):
    specs = [pl.BlockSpec(memory_space=pltpu.VMEM)] * len(args)
    if smem:
        specs[0] = pl.BlockSpec(memory_space=pltpu.SMEM)
    return pl.pallas_call(
        body,
        out_shape=tuple(outs),
        in_specs=specs,
        out_specs=tuple(pl.BlockSpec(memory_space=pltpu.VMEM) for _ in outs),
        scratch_shapes=list(scratch),
    )(*args)


def exchange(value_low, value_high, axis):
    return cyclic(value_high, axis, 1), cyclic(value_low, axis, -1)


def shards(right_side, guess):
    counts = tuple(lax.axis_size(a) for a in AXES)
    plan = Plan(right_side.shape, counts)
    nx, ny, nz = plan.local
    lanes = plan.lanes
    idx = jnp.stack([lax.axis_index(a) for a in AXES]).astype(jnp.int32)
    bind = lambda f, *extra: lambda *refs: f(plan, *extra, *refs)
    own = [sds(*n[:2], lanes) for n in plan.own[:HALO_LEVELS]]
    packs = [own[1], own[2], sds(plan.yrows, lanes), sds(plan.yrows, lanes), sds(plan.devices * plan.chunk, lanes)]

    xl, xu, yl, yu, zf = call(
        bind(faces_kernel), [sds(ny, lanes), sds(ny, lanes), sds(nx, lanes), sds(nx, lanes), sds(8, nx * ny)], [guess]
    )
    xlo, xhi = exchange(xl, xu, "gx")
    ylo, yhi = exchange(yl, yu, "gy")
    zlo, zhi = swap(zf)
    r, g1, g2, yl, yu, chunk = call(
        bind(residual_kernel),
        [own[0]] + packs,
        [idx, right_side, guess, xlo, xhi, ylo, yhi, zlo, zhi],
        [pltpu.VMEM((nx, ny, lanes), F32), plan.tmp],
        smem=True,
    )
    rings = [sds(*s) for s in plan.ring[:4]]
    as_scratch = lambda items: [pltpu.VMEM(s.shape, F32) for s in items]
    work = [pltpu.VMEM(s, F32) for s in plan.ring for _ in range(2)]
    work += [pltpu.VMEM(s, F32) for s in plan.ring[4:6]] + [plan.tmp]
    field, old = r, []
    kept = []
    for step in range(STEPS):
        last = step == STEPS - 1
        chunks = lax.all_to_all(chunk, AXES, 0, 0, tiled=True)
        ylo, yhi = exchange(yl, yu, "gy")
        *a, xl, xu = call(
            bind(ring_y_kernel),
            [sds(n[0], e[1], lanes) for n, e in zip(plan.own, plan.ext)] + [sds(plan.xrows, lanes)] * 2,
            [field, g1, g2, ylo, yhi],
        )
        xlo, xhi = exchange(xl, xu, "gx")
        *c, h = call(
            bind(ring_x_kernel),
            [sds(*e, lanes) for e in plan.ext] + [sds(8, sum(plan.hcols))],
            [*a, xlo, xhi],
        )
        hlo, hhi = swap(h)
        args = [idx, *c, hlo, hhi, chunks, *old]
        if last:
            z, w, sums = call(
                bind(step_kernel, True), [own[0], own[0], sds(plan.devices, lanes)], args, as_scratch(rings) + work, smem=True
            )
        else:
            z, w, g1, g2, yl, yu, chunk, *old = call(
                bind(step_kernel, False), [own[0], own[0]] + packs + rings, args, work, smem=True
            )
            field = w
        kept.append((z, w, chunks))
    sums = lax.all_to_all(sums, AXES, 0, 0, tiled=True)
    (z1, w1, _), (z2, w2, chunks1) = kept
    return call(bind(final_kernel), [own[0], own[0]], [chunks1, sums, guess, r, z1, w1, z2, w2])


def swap(h):
    low = cyclic(h, "gz", 1)
    return (low, low) if lax.axis_size("gz") == 2 else (low, cyclic(h, "gz", -1))


def solution(mesh):
    placed = P("gx", "gy", "gz")
    return jax.shard_map(shards, mesh=mesh, in_specs=(placed, placed), out_specs=(placed, placed), check_vma=False)
```

```python
import jax
import jax.numpy as jnp
from jax import lax
from jax.experimental import pallas as pl
from jax.experimental.pallas import tpu as pltpu
from jax.sharding import PartitionSpec as P

LEVELS = 6
SWEEPS = 4
STEPS = 2
M = SWEEPS
HALO_LEVELS = 3
AXES = ("gx", "gy", "gz")
F32 = jnp.float32
UNROLL = 24 * 24 * 128
HI = lax.Precision.HIGHEST


def up_to(value, unit):
    return -(-value // unit) * unit


def dot(a, b, dims=((1,), (0,))):
    return lax.dot_general(a, b, (dims, ((), ())), precision=HI, preferred_element_type=F32)


def pieces_of(x):
    high = x.astype(jnp.bfloat16).astype(F32)
    rest = x - high
    middle = rest.astype(jnp.bfloat16).astype(F32)
    return high, middle, rest - middle


def dot_right(x, hot):
    both = jnp.concatenate(pieces_of(x), axis=1).astype(jnp.bfloat16)
    return lax.dot_general(
        both, jnp.concatenate([hot, hot, hot], axis=0).astype(jnp.bfloat16), (((1,), (0,)), ((), ())), preferred_element_type=F32
    )


def dot_pick(hot, x):
    both = jnp.concatenate(pieces_of(x), axis=1).astype(jnp.bfloat16)
    return lax.dot_general(
        jnp.concatenate([hot, hot, hot], axis=1).astype(jnp.bfloat16), both, (((1,), (1,)), ((), ())), preferred_element_type=F32
    )


def dot_place(x, hot):
    both = jnp.concatenate(pieces_of(x), axis=0).astype(jnp.bfloat16)
    return lax.dot_general(
        both, jnp.concatenate([hot, hot, hot], axis=0).astype(jnp.bfloat16), (((0,), (0,)), ((), ())), preferred_element_type=F32
    )


def iota(shape, dim):
    return lax.broadcasted_iota(jnp.int32, shape, dim)


def one(cond):
    return jnp.where(cond, 1.0, 0.0).astype(F32)


def signed(index, size, own):
    return jnp.where(index < own + M, index, index - size)


def cyclic(value, axis, by):
    count = lax.axis_size(axis)
    return lax.ppermute(value, axis, [(i, (i + by) % count) for i in range(count)])


class Plan:
    def __init__(self, local, counts):
        self.local, self.counts = local, counts
        self.own = [tuple(n >> l for n in local) for l in range(LEVELS)]
        self.whole = [tuple(n * c >> l for n, c in zip(local, counts)) for l in range(LEVELS)]
        self.lanes = up_to(local[2], 128)
        self.ring = []
        for l in range(LEVELS):
            if l < HALO_LEVELS:
                n = self.own[l]
                self.ring.append((n[0] + 2 * M, up_to(n[1] + 2 * M, 8), up_to(n[2] + 2 * M, 128)))
            else:
                n = self.whole[l]
                self.ring.append((n[0] + 1, up_to(n[1] + 1, 8), up_to(n[2] + 1, 128)))
        self.devices = counts[0] * counts[1] * counts[2]
        self.chunk = self.own[HALO_LEVELS][1]
        self.ext = [(n[0] + 2 * M, n[1] + 2 * M) for n in self.own[:HALO_LEVELS]]
        self.tmp = pltpu.VMEM(
            (max(r[0] for r in self.ring), max(r[1] for r in self.ring), 128), F32
        )
        self.yrows = sum(n[0] * M for n in self.own[:HALO_LEVELS])
        self.xrows = sum(M * e[1] for e in self.ext)
        self.hcols = [up_to(e[0] * e[1], 128) for e in self.ext]


def restrict_to(plan, level, source, tmp):
    nx, ny, nz = plan.own[level]
    lanes = plan.lanes
    rz = one((iota((lanes, lanes), 0) >> 1 == iota((lanes, lanes), 1)) & (iota((lanes, lanes), 0) < nz)) * 0.125
    hx, hy = nx // 2, ny // 2
    for i in range(hx):
        tmp[i, 0:ny, 0:lanes] = source[2 * i] + source[2 * i + 1]
    pairs = tmp[0:hx, pl.ds(0, hy, stride=2), 0:lanes] + tmp[0:hx, pl.ds(1, hy, stride=2), 0:lanes]
    if hy % 8:
        return jnp.stack([dot_right(pairs[i], rz) for i in range(hx)])
    return dot_right(pairs.reshape(hx * hy, lanes), rz).reshape(hx, hy, lanes)


def send_pack(plan, v, g1, g2, yl, yu, chunk, sums, tmp):
    lanes = plan.lanes
    g1[...] = restrict_to(plan, 0, v, tmp)
    g2[...] = restrict_to(plan, 1, g1, tmp)
    n3 = plan.own[3]
    coarse = restrict_to(plan, 2, g2, tmp)
    parts = [jnp.zeros((n3[1], lanes), F32)]
    for i in range(n3[0]):
        parts[0] = parts[0] + (pltpu.roll(coarse[i], i * n3[2], 1) if i else coarse[i])
    payload = parts[0]
    if sums is not None:
        at = iota(payload.shape, 1)
        first = iota(payload.shape, 0) == 0
        payload = jnp.where((at == lanes - 2) & first, sums[0], payload)
        payload = jnp.where((at == lanes - 1) & first, sums[1], payload)
    for d in range(plan.devices):
        chunk[d * plan.chunk : (d + 1) * plan.chunk, :] = payload
    row = 0
    for l, f in enumerate((v, g1, g2)):
        nx, ny, _ = plan.own[l]
        for i in range(nx):
            yl[row : row + M, :] = f[i, 0:M, :]
            yu[row : row + M, :] = f[i, ny - M : ny, :]
            row += M


def inside(plan, idx, level, dim, ring_index):
    size = plan.ring[level][dim]
    if level < HALO_LEVELS:
        own = plan.own[level][dim]
        at = signed(ring_index, size, own) + idx[dim] * own
        ok = (at >= 0) & (at < plan.whole[level][dim])
        s = signed(ring_index, size, own)
        return ok & (s >= -M)
    return ring_index < plan.whole[level][dim]


def plane_mask(plan, idx, level):
    _, ry, rz = plan.ring[level]
    return one(
        inside(plan, idx, level, 1, iota((ry, rz), 0)) & inside(plan, idx, level, 2, iota((ry, rz), 1))
    )


def smooth(plan, idx, level, g, a, b):
    rx, ry, rz = plan.ring[level]
    m9 = plane_mask(plan, idx, level) * (1.0 / 9.0)
    source, target = g, a
    for sweep in range(SWEEPS - 1):

        group = rx if rx * ry * rz <= UNROLL else max(u for u in range(1, 9) if rx % u == 0)

        def plane(i, source=source, target=target):
            fixed = isinstance(i, int)
            f = source[i]
            before = source[(i - 1) % rx if fixed else jnp.where(i == 0, rx - 1, i - 1)]
            after = source[(i + 1) % rx if fixed else jnp.where(i == rx - 1, 0, i + 1)]
            beside = before + after + pltpu.roll(f, 1, 0) + pltpu.roll(f, ry - 1, 0)
            beside = beside + pltpu.roll(f, 1, 1) + pltpu.roll(f, rz - 1, 1)
            sx = one(inside(plan, idx, level, 0, jnp.int32(i)))
            target[i] = g[i] + (m9 * sx) * (3.0 * f + beside)

        def body(j, carry, plane=plane, group=group):
            for u in range(group):
                plane(j * group + u)
            return carry

        if group == rx:
            for i in range(rx):
                plane(i)
        else:
            lax.fori_loop(0, rx // group, body, 0)
        source, target = target, (b if target is a else a)
    return source


def coarse_map(plan, idx, level, dim, fine, coarse):
    size = plan.ring[level][dim]
    if level < HALO_LEVELS:
        s = signed(fine, size, plan.own[level][dim])
        if level + 1 < HALO_LEVELS:
            up = s >> 1
            return jnp.where(up < 0, up + plan.ring[level + 1][dim], up) == coarse
        return (s + idx[dim] * plan.own[level][dim]) >> 1 == coarse
    return (fine >> 1 == coarse) & (fine < plan.whole[level][dim])


def add_prolonged(plan, idx, level, f, scale, zc, out, tmp):
    rx, ry, rz = plan.ring[level]
    cx, cy, cz = plan.ring[level + 1]
    pz = one(coarse_map(plan, idx, level, 2, iota((cz, rz), 1), iota((cz, rz), 0)))
    halo = level < HALO_LEVELS
    low = -1 if halo else 0
    high = plan.own[level][0] + 1 if halo else plan.whole[level][0]
    planes = range(low >> 1, (high - 1 >> 1) + 1)
    if level + 1 == HALO_LEVELS:
        py = one(coarse_map(plan, idx, level, 1, iota((ry, cy), 0), iota((ry, cy), 1)))
        for k in planes:
            at = k + idx[0] * (plan.own[level][0] // 2)
            ok = (at >= 0) & (at < plan.whole[level + 1][0])
            c = jnp.clip(at, 0, plan.whole[level + 1][0] - 1)
            u = dot(py, dot_right(zc[c], pz)) * one(ok)
            for s in (2 * k, 2 * k + 1):
                if low <= s < high:
                    out[s % rx] = scale * f[s % rx] + u
        return
    upper = (plan.own[level][1] + M) // 2 if halo else ry // 2
    for n, k in enumerate(planes):
        for odd in (0, 1):
            tmp[n, pl.ds(odd, upper, stride=2), 0:cz] = zc[k % cx, 0:upper, :]
            if halo:
                tmp[n, pl.ds(2 * upper + odd, M // 2, stride=2), 0:cz] = zc[k % cx, cy - M // 2 : cy, :]
    spread = dot_right(tmp[0 : len(planes), 0:ry, 0:cz].reshape(len(planes) * ry, cz), pz).reshape(len(planes), ry, rz)
    for n, k in enumerate(planes):
        for s in (2 * k, 2 * k + 1):
            if low <= s < high:
                out[s % rx] = scale * f[s % rx] + spread[n]
    if not halo:
        for i in range(high, rx):
            out[i] = jnp.zeros((ry, rz), F32)


def faces_kernel(plan, guess, xl, xu, yl, yu, zf):
    nx, ny, nz = plan.local
    lanes = plan.lanes
    xl[...] = guess[0]
    xu[...] = guess[nx - 1]
    yl[...] = guess[:, 0, :]
    yu[...] = guess[:, ny - 1, :]
    at, row = iota((8, lanes), 1), iota((8, lanes), 0)
    pick = one(((row == 0) & (at == 0)) | ((row == 1) & (at == nz - 1)))
    zf[...] = dot_pick(pick, guess[...].reshape(nx * ny, lanes))


def residual_kernel(plan, idx, b, guess, xlo, xhi, ylo, yhi, zlo, zhi, r, g1, g2, yl, yu, chunk, side, tmp):
    nx, ny, nz = plan.local
    lanes = plan.lanes
    cx, cy, cz = plan.counts
    has = lambda dim, upper: one(idx[dim] < plan.counts[dim] - 1 if upper else idx[dim] > 0)
    at, row = iota((8, lanes), 1), iota((8, lanes), 0)
    upper = one((row == 0) & (at == nz - 1)) * has(2, True)
    lower = one((row == 1) & (at == 0)) * has(2, False)
    got = jnp.where(iota((8, nx * ny), 0) == 0, zhi[...], zlo[...])
    side[...] = dot_place(got, upper + lower).reshape(nx, ny, lanes)
    ys, zs = iota((ny, lanes), 0), iota((ny, lanes), 1)
    not_low, not_high = one(zs > 0), one(zs < nz - 1)
    y_low, y_high = ys == 0, ys == ny - 1
    for i in range(nx):
        f = guess[i]
        before = guess[i - 1] if i else xlo[...] * has(0, False)
        after = guess[i + 1] if i < nx - 1 else xhi[...] * has(0, True)
        beside = before + after
        beside = beside + jnp.where(y_low, (ylo[i] * has(1, False))[None, :], pltpu.roll(f, 1, 0))
        beside = beside + jnp.where(y_high, (yhi[i] * has(1, True))[None, :], pltpu.roll(f, ny - 1, 0))
        beside = beside + pltpu.roll(f, 1, 1) * not_low + pltpu.roll(f, lanes - 1, 1) * not_high
        r[i] = b[i] - (6.0 * f - (beside + side[i]))
    send_pack(plan, r, g1, g2, yl, yu, chunk, None, tmp)


def ring_y_kernel(plan, v, g1, g2, ylo, yhi, a0, a1, a2, xl, xu):
    row, out = 0, 0
    for l, (f, a) in enumerate(((v, a0), (g1, a1), (g2, a2))):
        nx, ny, _ = plan.own[l]
        e = plan.ext[l][1]
        a[:, 0:ny, :] = f[...]
        for i in range(nx):
            a[i, ny : ny + M, :] = yhi[row : row + M, :]
            a[i, ny + M : ny + 2 * M, :] = ylo[row : row + M, :]
            row += M
        for i in range(M):
            xl[out : out + e, :] = a[i]
            xu[out : out + e, :] = a[nx - M + i]
            out += e


def ring_x_kernel(plan, a0, a1, a2, xlo, xhi, c0, c1, c2, h):
    row, col = 0, 0
    lanes = plan.lanes
    at, k = iota((8, lanes), 1), iota((8, lanes), 0)
    for l, (a, c) in enumerate(((a0, c0), (a1, c1), (a2, c2))):
        nx, ny, nz = plan.own[l]
        ex, e = plan.ext[l]
        c[0:nx] = a[...]
        for i in range(M):
            c[nx + i] = xhi[row : row + e, :]
            c[nx + M + i] = xlo[row : row + e, :]
            row += e
        pick = one(at == jnp.where(k < M, k, nz - 2 * M + k))
        h[:, col : col + ex * e] = dot_pick(pick, c[...].reshape(ex * e, lanes))
        if plan.hcols[l] > ex * e:
            h[:, col + ex * e : col + plan.hcols[l]] = jnp.zeros((8, plan.hcols[l] - ex * e), F32)
        col += plan.hcols[l]


def total_sums(plan, chunks):
    rows = chunks.shape
    at = iota(rows, 1)
    first = iota(rows, 0) % plan.chunk == 0
    data = chunks[...]
    along = jnp.sum(jnp.where((at == plan.lanes - 2) & first, data, 0.0))
    curvature = jnp.sum(jnp.where((at == plan.lanes - 1) & first, data, 0.0))
    return along, curvature


def step_kernel(plan, last, *refs):
    nin = 7 if not last else 11
    idx, c0, c1, c2, hlo, hhi, chunks = refs[:7]
    old = refs[7:nin]
    outs = refs[nin:]
    if last:
        z_out, w_out, sums_out = outs[:3]
        scratch = outs[3:]
        rings = scratch[:4]
        scratch = scratch[4:]
    else:
        z_out, w_out, g1, g2, yl, yu, chunk = outs[:7]
        rings = outs[7:11]
        scratch = outs[11:]
    bufs = [scratch[2 * l : 2 * l + 2] for l in range(LEVELS)]
    g4, g5, tmp = scratch[2 * LEVELS : 2 * LEVELS + 3]
    fields = list(rings) + [g4, g5]
    lanes = plan.lanes
    if last:
        along, curvature = total_sums(plan, chunks)
        alpha = along / curvature
    col = 0
    at, k = iota((8, lanes), 1), iota((8, lanes), 0)
    for l, c in enumerate((c0, c1, c2)):
        nx, ny, nz = plan.own[l]
        ex, e = plan.ext[l]
        rx, ry, rz = plan.ring[l]
        mask = plane_mask(plan, idx, l)
        base = rz - lanes
        want = jnp.where(k < M, nz + k - base, lanes - 2 * M + k)
        place = one(at == want)
        got = jnp.where(iota((8, ex * e), 0) < M, hhi[:, col : col + ex * e], hlo[:, col : col + ex * e])
        col += plan.hcols[l]
        tile = dot_place(got, place).reshape(ex, e, lanes)
        for i in range(rx):
            m = mask * one(inside(plan, idx, l, 0, jnp.int32(i)))
            if base:
                full = jnp.concatenate([c[i], tile[i]], axis=1)
            else:
                full = c[i] + tile[i]
            full = full * m
            rings[l][i] = old[l][i] - alpha * full if last else full
    n3 = plan.own[3]
    g3 = rings[3]
    g3[...] = jnp.zeros(g3.shape, F32)
    d = 0
    for ix in range(plan.counts[0]):
        for iy in range(plan.counts[1]):
            for iz in range(plan.counts[2]):
                part = chunks[d * plan.chunk : (d + 1) * plan.chunk, :]
                for i in range(n3[0]):
                    g3[
                        ix * n3[0] + i, iy * n3[1] : (iy + 1) * n3[1], iz * n3[2] : (iz + 1) * n3[2]
                    ] = part[:, i * n3[2] : (i + 1) * n3[2]]
                d += 1
    if last:
        g3[...] = old[3][...] - alpha * g3[...]
    for l in (3, 4):
        rx, ry, rz = plan.ring[l]
        cx, cy, cz = plan.ring[l + 1]
        rzm = one((iota((rz, cz), 0) >> 1 == iota((rz, cz), 1)) & (iota((rz, cz), 0) < plan.whole[l][2])) * 0.125
        hx, hy = plan.whole[l + 1][:2]
        fields[l + 1][...] = jnp.zeros((cx, cy, cz), F32)
        for i in range(hx):
            both = fields[l][2 * i] + fields[l][2 * i + 1]
            pieces = []
            for t in range(0, rz, 128):
                n = i * (rz // 128) + t // 128
                tmp[n, 0:ry, :] = both[:, t : t + 128]
                pieces.append(tmp[n, pl.ds(0, ry // 2, stride=2), :] + tmp[n, pl.ds(1, ry // 2, stride=2), :])
            pair = jnp.concatenate(pieces, axis=1)
            fields[l + 1][i, 0 : ry // 2, :] = dot_right(pair, rzm)
    zc = None
    for l in range(LEVELS - 1, -1, -1):
        f = smooth(plan, idx, l, fields[l], *bufs[l])
        out = bufs[l][1] if f is bufs[l][0] else bufs[l][0]
        scale = 4.0**l / 9.0
        if zc is None:
            out[...] = scale * f[...]
        else:
            add_prolonged(plan, idx, l, f, scale, zc, out, tmp)
        zc = out
    nx, ny, nz = plan.local
    rx, ry, rz = plan.ring[0]
    first = jnp.zeros((ny, lanes), F32)
    second = jnp.zeros((ny, lanes), F32)

    group = max(u for u in range(1, 5) if nx % u == 0)

    def body(j, carry):
        first, second = carry
        for u in range(group):
            i = j * group + u
            f = zc[i]
            before = zc[jnp.where(i == 0, rx - 1, i - 1)]
            after = zc[i + 1]
            beside = before + after + pltpu.roll(f, 1, 0) + pltpu.roll(f, ry - 1, 0)
            beside = beside + pltpu.roll(f, 1, 1) + pltpu.roll(f, rz - 1, 1)
            w = (6.0 * f - beside)[:ny, :lanes]
            z = f[:ny, :lanes]
            z_out[i] = z
            w_out[i] = w
            first = first + z * rings[0][i][:ny, :lanes]
            second = second + z * w
        return first, second

    first, second = lax.fori_loop(0, nx // group, body, (first, second))
    sums = (jnp.sum(first), jnp.sum(second))
    if last:
        row, at = iota(sums_out.shape, 0), iota(sums_out.shape, 1)
        sums_out[...] = jnp.where(at == lanes - 2, sums[0], jnp.where(at == lanes - 1, sums[1], 0.0))
    else:
        send_pack(plan, w_out, g1, g2, yl, yu, chunk, sums, tmp)


def final_kernel(plan, chunks1, chunks2, guess, r, z1, w1, z2, w2, x_out, r_out):
    along, curvature = total_sums(plan, chunks1)
    alpha1 = along / curvature
    data = chunks2[...]
    at = iota(data.shape, 1)
    along = jnp.sum(jnp.where(at == plan.lanes - 2, data, 0.0))
    curvature = jnp.sum(jnp.where(at == plan.lanes - 1, data, 0.0))
    alpha2 = along / curvature
    x_out[...] = guess[...] + alpha1 * z1[...] + alpha2 * z2[...]
    r_out[...] = r[...] - alpha1 * w1[...] - alpha2 * w2[...]


def sds(*shape):
    return jax.ShapeDtypeStruct(shape, F32)


def call(body, outs, args, scratch=(), smem=False):
    specs = [pl.BlockSpec(memory_space=pltpu.VMEM)] * len(args)
    if smem:
        specs[0] = pl.BlockSpec(memory_space=pltpu.SMEM)
    return pl.pallas_call(
        body,
        out_shape=tuple(outs),
        in_specs=specs,
        out_specs=tuple(pl.BlockSpec(memory_space=pltpu.VMEM) for _ in outs),
        scratch_shapes=list(scratch),
    )(*args)


def exchange(value_low, value_high, axis):
    return cyclic(value_high, axis, 1), cyclic(value_low, axis, -1)


def shards(right_side, guess):
    counts = tuple(lax.axis_size(a) for a in AXES)
    plan = Plan(right_side.shape, counts)
    nx, ny, nz = plan.local
    lanes = plan.lanes
    idx = jnp.stack([lax.axis_index(a) for a in AXES]).astype(jnp.int32)
    bind = lambda f, *extra: lambda *refs: f(plan, *extra, *refs)
    own = [sds(*n[:2], lanes) for n in plan.own[:HALO_LEVELS]]
    packs = [own[1], own[2], sds(plan.yrows, lanes), sds(plan.yrows, lanes), sds(plan.devices * plan.chunk, lanes)]

    xl, xu, yl, yu, zf = call(
        bind(faces_kernel), [sds(ny, lanes), sds(ny, lanes), sds(nx, lanes), sds(nx, lanes), sds(8, nx * ny)], [guess]
    )
    xlo, xhi = exchange(xl, xu, "gx")
    ylo, yhi = exchange(yl, yu, "gy")
    zlo, zhi = swap(zf)
    r, g1, g2, yl, yu, chunk = call(
        bind(residual_kernel),
        [own[0]] + packs,
        [idx, right_side, guess, xlo, xhi, ylo, yhi, zlo, zhi],
        [pltpu.VMEM((nx, ny, lanes), F32), plan.tmp],
        smem=True,
    )
    rings = [sds(*s) for s in plan.ring[:4]]
    as_scratch = lambda items: [pltpu.VMEM(s.shape, F32) for s in items]
    work = [pltpu.VMEM(s, F32) for s in plan.ring for _ in range(2)]
    work += [pltpu.VMEM(s, F32) for s in plan.ring[4:6]] + [plan.tmp]
    field, old = r, []
    kept = []
    for step in range(STEPS):
        last = step == STEPS - 1
        chunks = lax.all_to_all(chunk, AXES, 0, 0, tiled=True)
        ylo, yhi = exchange(yl, yu, "gy")
        *a, xl, xu = call(
            bind(ring_y_kernel),
            [sds(n[0], e[1], lanes) for n, e in zip(plan.own, plan.ext)] + [sds(plan.xrows, lanes)] * 2,
            [field, g1, g2, ylo, yhi],
        )
        xlo, xhi = exchange(xl, xu, "gx")
        *c, h = call(
            bind(ring_x_kernel),
            [sds(*e, lanes) for e in plan.ext] + [sds(8, sum(plan.hcols))],
            [*a, xlo, xhi],
        )
        hlo, hhi = swap(h)
        args = [idx, *c, hlo, hhi, chunks, *old]
        if last:
            z, w, sums = call(
                bind(step_kernel, True), [own[0], own[0], sds(plan.devices, lanes)], args, as_scratch(rings) + work, smem=True
            )
        else:
            z, w, g1, g2, yl, yu, chunk, *old = call(
                bind(step_kernel, False), [own[0], own[0]] + packs + rings, args, work, smem=True
            )
            field = w
        kept.append((z, w, chunks))
    sums = lax.all_to_all(sums, AXES, 0, 0, tiled=True)
    (z1, w1, _), (z2, w2, chunks1) = kept
    return call(bind(final_kernel), [own[0], own[0]], [chunks1, sums, guess, r, z1, w1, z2, w2])


def swap(h):
    low = cyclic(h, "gz", 1)
    return (low, low) if lax.axis_size("gz") == 2 else (low, cyclic(h, "gz", -1))


def solution(mesh):
    placed = P("gx", "gy", "gz")
    return jax.shard_map(shards, mesh=mesh, in_specs=(placed, placed), out_specs=(placed, placed), check_vma=False)
```
